256 devices in a mesh: section: 2 (over core), row: 16 (over y, x), col: 8 (over z).
Axes of the slice: x: 4, y: 4, z: 8, core: 2. Of those that a mesh axis runs over, the one named last changes fastest.
Arguments:
- section_inputs: bfloat16 [2, 2, 192, 4096], P('section', None, 'col', 'row'), may hold values from -6 to 6
- out_grad: bfloat16 [2, 192, 4096], P(None, 'col', 'row'), may hold values from -6 to 6
- gate_weight: bfloat16 [2, 4096, 14336], P('section', 'row', 'col'), may hold values from -0.09375 to 0.09375
- up_weight: bfloat16 [2, 4096, 14336], P('section', 'row', 'col'), may hold values from -0.09375 to 0.09375
- down_weight: bfloat16 [2, 14336, 4096], P('section', 'col', 'row'), may hold values from -0.046875 to 0.046875
Outputs:
- input_grads: bfloat16 [2, 2, 192, 4096], P('section', None, 'col', 'row')
- grad_gate: float32 [2, 4096, 14336], P('section', 'row', 'col')
- grad_up: float32 [2, 4096, 14336], P('section', 'row', 'col')
- grad_down: float32 [2, 14336, 4096], P('section', 'col', 'row')
The draws below stay inside these ranges and needn't reach their ends.
All inputs are finite; a program needn't handle non-finite values.
Results may differ from the reference program's by a relative error of at most 0.025.
Values may be sent and summed in bfloat16 or wider, within the bound.
A program may use at most 64 MiB of HBM per device.

```python
import jax
import jax.numpy as jnp

D = 4096
FF = 14336
MICRO = 2
SECTIONS = 2
TOKENS = 192
N_ROW = 16


def level_of(own_key, shape, pieces, low, top_value):
    gain, own = 1.0, jax.random.fold_in(own_key, 6)
    for position, shards_of in pieces:
        steps = jnp.exp(jax.random.uniform(jax.random.fold_in(own, position), (shards_of,), jnp.float32, low / len(pieces), top_value / len(pieces)))
        gain = gain * jnp.repeat(steps, shape[position] // shards_of).reshape([-1 if axis == position else 1 for axis in range(len(shape))])
    return gain


def gaussian(own_key, extent, scale, most, cuts=(), dtype=jnp.bfloat16):
    result = scale * jax.random.normal(own_key, extent, jnp.float32)
    if cuts:
        result = result * level_of(own_key, extent, cuts, -0.22, 0.18)
    return jnp.clip(result, -most, most).astype(dtype)


def setup_inputs(seed: int = 0) -> dict:
    arg_keys = jax.random.split(jax.random.key(seed), 6)
    section_inputs = gaussian(arg_keys[0], (SECTIONS, MICRO, TOKENS, D), 1.0, 6.0, ((0, 2), (2, 8), (3, 16)))
    out_grad = gaussian(arg_keys[1], (MICRO, TOKENS, D), 1.0, 6.0, ((1, 8), (2, 16)))
    gate_weight = gaussian(arg_keys[2], (SECTIONS, D, FF), D ** -0.5, 0.09375, ((0, 2), (1, 16), (2, 8)))
    up_weight = gaussian(arg_keys[3], (SECTIONS, D, FF), D ** -0.5, 0.09375, ((0, 2), (1, 16), (2, 8)))
    down_weight = gaussian(arg_keys[4], (SECTIONS, FF, D), FF ** -0.5, 0.046875, ((0, 2), (1, 8), (2, 16)))
    return dict(section_inputs=section_inputs, out_grad=out_grad, gate_weight=gate_weight, up_weight=up_weight, down_weight=down_weight)


def blocked_sum(left, right):
    width = D // N_ROW
    total = jnp.zeros((left.shape[0], right.shape[1]), jnp.float32)
    for block in range(N_ROW):
        piece = jnp.dot(left[:, block * width:(block + 1) * width], right[block * width:(block + 1) * width],
                        preferred_element_type=jnp.float32).astype(jnp.bfloat16)
        total = total + piece.astype(jnp.float32)
    return total


def layer_backward(x_rows, dy_rows, w_gate, w_up, w_down):
    gate_sum = blocked_sum(x_rows, w_gate)
    up_sum = blocked_sum(x_rows, w_up)
    sigmoid_gate = jax.nn.sigmoid(gate_sum)
    activated = gate_sum * sigmoid_gate
    slope = sigmoid_gate * (1.0 + gate_sum * (1.0 - sigmoid_gate))
    hidden = (activated * up_sum).astype(jnp.bfloat16)
    hidden_grad = blocked_sum(dy_rows, w_down.T)
    gate_grad = (hidden_grad * up_sum * slope).astype(jnp.bfloat16)
    up_grad = (hidden_grad * activated).astype(jnp.bfloat16)
    branch = jnp.dot(gate_grad, w_gate.T, preferred_element_type=jnp.float32)
    branch = branch + jnp.dot(up_grad, w_up.T, preferred_element_type=jnp.float32)
    input_grad = (dy_rows.astype(jnp.float32) + branch).astype(jnp.bfloat16)
    gate_update = jnp.dot(x_rows.T, gate_grad, preferred_element_type=jnp.float32)
    up_update = jnp.dot(x_rows.T, up_grad, preferred_element_type=jnp.float32)
    down_update = jnp.dot(hidden.T, dy_rows, preferred_element_type=jnp.float32)
    return input_grad, gate_update, up_update, down_update


def reference(section_inputs, out_grad, gate_weight, up_weight, down_weight):
    carried = [out_grad[micro_index] for micro_index in range(MICRO)]
    input_list = []
    gate_list = []
    up_list = []
    down_list = []
    for section_number in reversed(range(SECTIONS)):
        gate_total = jnp.zeros((D, FF), jnp.float32)
        up_total = jnp.zeros((D, FF), jnp.float32)
        down_total = jnp.zeros((FF, D), jnp.float32)
        produced = []
        for micro_index in range(MICRO):
            input_grad, gate_update, up_update, down_update = layer_backward(
                section_inputs[section_number, micro_index], carried[micro_index],
                gate_weight[section_number], up_weight[section_number], down_weight[section_number])
            produced.append(input_grad)
            gate_total = gate_total + gate_update
            up_total = up_total + up_update
            down_total = down_total + down_update
        carried = produced
        input_list.insert(0, jnp.stack(produced))
        gate_list.insert(0, gate_total)
        up_list.insert(0, up_total)
        down_list.insert(0, down_total)
    return jnp.stack(input_list), jnp.stack(gate_list), jnp.stack(up_list), jnp.stack(down_list)
```

```python
import functools

import jax
import jax.numpy as jnp
from jax import lax
from jax.experimental import pallas as pl
from jax.experimental.pallas import tpu as pltpu
from jax.sharding import PartitionSpec as P

MESH = pl.DeviceIdType.MESH
BF16 = jnp.bfloat16
F32 = jnp.float32
RING = 4
GATE, UP, DHID = 0, 1, 2
HIDDEN, DGATE, DUP = 0, 1, 2
NT_DIMS = (((1,), (1,)), ((), ()))
TN_DIMS = (((0,), (0,)), ((), ()))


def relay_kernel(
    n_col,
    x_ref, dy_ref, wg_hbm, wu_hbm, wd_hbm,
    out_ref, h_hbm, xall_hbm, dyall_hbm,
    wg, wu, wd, xall, dyall, part, ra, rb, ra2, rb2, final, gath, factors, acc, dxp, rz, blk_out,
    load_sem, store_sem,
    rs_send, rs_recv, ag_send, ag_recv, zx_send, zx_recv, zy_send, zy_recv, zr_send, zr_recv, zo_send, zo_recv,
):
    sec = lax.axis_index("section")
    row = lax.axis_index("row")
    col = lax.axis_index("col")
    gx = lax.rem(row, RING)
    gy = lax.div(row, RING)
    tok_loc = x_ref.shape[0]
    tok = xall.shape[0]
    tiles = wg.shape[1] // 256
    blk = tok // RING
    sub = blk // RING
    half = blk // 2
    ta = (tiles + 1) // 2

    def step(pos, d):
        return lax.rem(pos + (d + RING), RING)

    def along_x(d):
        return (sec, gy * RING + step(gx, d), col)

    def along_y(d):
        return (sec, step(gy, d) * RING + gx, col)

    def z_peer(d):
        return lax.rem(col + d, n_col)

    pos1 = (gx, gy)
    pos2 = (gy, gx)
    ring1 = (along_x, along_y)
    ring2 = (along_y, along_x)

    weights = ((wg_hbm, wg), (wu_hbm, wu), (wd_hbm, wd))
    loads = [pltpu.make_async_copy(s, d, load_sem.at[i]) for i, (s, d) in enumerate(weights)]
    for c in loads:
        c.start()

    barrier = pltpu.get_barrier_semaphore()
    greeted = [along_x(1), along_x(-1), along_y(1), along_y(-1)]
    greeted += [(sec, row, z_peer(d)) for d in range(1, n_col)]
    greeted += [(1 - sec, row, z_peer(d)) for d in range(n_col)]
    for dev in greeted:
        pl.semaphore_signal(barrier, inc=1, device_id=dev, device_id_type=MESH)
    pl.semaphore_wait(barrier, len(greeted))

    def rcopy(src, dst, ssem, rsem, dev):
        return pltpu.make_async_remote_copy(
            src_ref=src, dst_ref=dst, send_sem=ssem, recv_sem=rsem, device_id=dev, device_id_type=MESH
        )

    def aligned(v, m=8):
        return pl.multiple_of(v, m)

    my_rows = pl.ds(aligned(col * tok_loc), tok_loc)

    def spread(src, dst, ssem, rsem):
        sent = []
        for d in range(1, n_col):
            c = rcopy(src, dst.at[my_rows, :], ssem.at[d], rsem.at[d], (sec, row, z_peer(d)))
            c.start()
            sent.append(c)
        return sent

    def region1(ref, k, h, q, part_ab):
        return ref.at[k, h, :, pl.ds(aligned(q * blk + part_ab * half), half), :]

    def region2(ref, k, h, q, part_ab):
        t = pl.ds(0, ta) if part_ab == 0 else pl.ds(ta, tiles - ta)
        return ref.at[k, h, t, pl.ds(aligned(pos1[h] * blk + q * sub), sub), :]

    def recv1(k, h, way, part_ab):
        return rb.at[k, h, way, :, pl.ds(part_ab * half, half), :]

    def recv2(k, h, way, part_ab):
        t = pl.ds(0, ta) if part_ab == 0 else pl.ds(ta, tiles - ta)
        return rb2.at[k, h, way, t, :, :]

    def early1(k, h, way):
        return ra.at[k, h, way]

    def early2(k, h, way):
        t = pl.ds(0, ta) if way == 0 else pl.ds(ta, tiles - ta)
        return ra2.at[k, h, t, :, :]

    stages = (
        (pos1, ring1, region1, recv1, early1),
        (pos2, ring2, region2, recv2, early2),
    )

    def rs_copy(k, h, st, way, kind):
        pos, ring, region, recv, early = stages[st]
        d = 1 if way == 0 else -1
        ssem, rsem = rs_send.at[k, h, st, way, kind], rs_recv.at[k, h, st, way, kind]
        if kind == 0:
            src, dst = region(part, k, h, step(pos[h], 2), way), early(k, h, way)
        else:
            ab = way if kind == 2 else 1 - way
            src, dst = region(part, k, h, step(pos[h], d), ab), recv(k, h, way, ab)
        return rcopy(src, dst, ssem, rsem, ring[h](d))

    def rs_start(k, st):
        for kind in (0, 1):
            for h in range(2):
                for way in range(2):
                    rs_copy(k, h, st, way, kind).start()

    def add_into(dst, src):
        def body(t, _):
            dst[t] = (dst[t].astype(F32) + src[t].astype(F32)).astype(BF16)
            return 0

        lax.fori_loop(0, dst.shape[0], body, 0)

    def rs_mid(k, st):
        pos, ring, region, recv, early = stages[st]
        for h in range(2):
            for way in range(2):
                d = 1 if way == 0 else -1
                rs_copy(k, h, st, way, 0).wait_recv()
                add_into(region(part, k, h, step(pos[h], d), way), early(k, h, way))
                rs_copy(k, h, st, way, 2).start()

    def rs_wait(k, st):
        for h in range(2):
            for kind in (1, 2):
                for way in range(2):
                    rs_copy(k, h, st, way, kind).wait_recv()

    def rs_end1(k):
        rs_wait(k, 0)
        for h in range(2):
            own = part.at[k, h, :, pl.ds(aligned(pos1[h] * blk), blk), :]
            a, b = rb.at[k, h, 0], rb.at[k, h, 1]

            def body(t, _):
                own[t] = (own[t].astype(F32) + (a[t].astype(F32) + b[t].astype(F32))).astype(BF16)
                return 0

            lax.fori_loop(0, tiles, body, 0)

    def piece(ref, k, h):
        return ref.at[k, h, :, pl.ds(aligned(pos1[h] * blk + pos2[h] * sub), sub), :]

    def rs_end2(k):
        rs_wait(k, 1)
        for h in range(2):
            own, a, b, f = piece(part, k, h), rb2.at[k, h, 0], rb2.at[k, h, 1], final.at[k, h]

            def body(t, _):
                f[t] = own[t].astype(F32) + (a[t].astype(F32) + b[t].astype(F32))
                return 0

            lax.fori_loop(0, tiles, body, 0)

    def rs_drain(k):
        for st in range(2):
            for h in range(2):
                for way in range(2):
                    for kind in range(3):
                        rs_copy(k, h, st, way, kind).wait_send()

    def reduce_rows(ks):
        for k in ks:
            rs_mid(k, 0)
        for k in ks:
            rs_end1(k)
            rs_start(k, 1)
        for k in ks:
            rs_mid(k, 1)
        for k in ks:
            rs_end2(k)

    def ag_copy(k, h, st, way, kind):
        pos, ring, region, _, _ = stages[st]
        d = 1 if way == 0 else -1
        ssem, rsem = ag_send.at[k, h, st, way, kind], ag_recv.at[k, h, st, way, kind]
        ab = 1 - way if kind == 1 else way
        q = pos[h] if kind < 2 else step(pos[h], -d)
        ref = region(gath, k, h, q, ab)
        return rcopy(ref, ref, ssem, rsem, ring[h](d))

    def ag_start(k, st):
        for kind in (0, 1):
            for h in range(2):
                for way in range(2):
                    ag_copy(k, h, st, way, kind).start()

    def ag_mid(k, st):
        for h in range(2):
            for way in range(2):
                ag_copy(k, h, st, way, 0).wait_recv()
                ag_copy(k, h, st, way, 2).start()

    def ag_end(k, st):
        for h in range(2):
            for kind in (1, 2):
                for way in range(2):
                    ag_copy(k, h, st, way, kind).wait_recv()

    def ag_drain(k):
        for st in range(2):
            for h in range(2):
                for way in range(2):
                    for kind in range(3):
                        ag_copy(k, h, st, way, kind).wait_send()

    def gather_rows(ks):
        for k in ks:
            ag_start(k, 1)
        for k in ks:
            ag_mid(k, 1)
        for k in ks:
            ag_end(k, 1)
            ag_start(k, 0)
        for k in ks:
            ag_mid(k, 0)
        for k in ks:
            ag_end(k, 0)

    def partials(k):
        def body(t, _):
            cols = pl.ds(pl.multiple_of(t * 256, 256), 256)
            if k == DHID:
                o = lax.dot_general(dyall[...], wd[cols, :], NT_DIMS, preferred_element_type=F32)
            else:
                w = wg if k == GATE else wu
                o = jnp.dot(xall[...], w[:, cols], preferred_element_type=F32)
            part[k, 0, t] = o[:, :128].astype(BF16)
            part[k, 1, t] = o[:, 128:].astype(BF16)
            return 0

        lax.fori_loop(0, tiles, body, 0)

    def swiglu(gate, up):
        sig = 1.0 / (1.0 + jnp.exp(-gate))
        act = gate * sig
        return act, up * (sig * (1.0 + gate * (1.0 - sig)))

    def exchange_cols():
        sent = []
        for d in range(1, n_col):
            peer = z_peer(d)
            c = rcopy(
                dxp.at[pl.ds(aligned(peer * tok_loc), tok_loc), :], rz.at[d], zr_send.at[d], zr_recv.at[d], (sec, row, peer)
            )
            c.start()
            sent.append(c)
        total = acc[my_rows, :]
        for c in sent:
            c.wait_recv()
        for d in range(1, n_col):
            total = total + rz[d].astype(F32)
        return total, sent

    def copies_out(src):
        out = [
            pltpu.make_async_copy(src, h_hbm, store_sem.at[0]),
            pltpu.make_async_copy(xall, xall_hbm, store_sem.at[1]),
            pltpu.make_async_copy(dyall, dyall_hbm, store_sem.at[2]),
        ]
        for c in out:
            c.start()
        return out

    xall[my_rows, :] = x_ref[...]

    @pl.when(sec == 1)
    def _():
        dyall[my_rows, :] = dy_ref[...]
        sent = spread(dy_ref, dyall, zy_send, zy_recv)
        sent_x = spread(x_ref, xall, zx_send, zx_recv)
        for c in loads:
            c.wait()
        for c in sent:
            c.wait_recv()
        partials(DHID)
        rs_start(DHID, 0)
        for c in sent_x:
            c.wait_recv()
        for k in (GATE, UP):
            partials(k)
            rs_start(k, 0)
        reduce_rows((DHID, GATE, UP))
        for h in range(2):
            outs = [piece(gath, k, h) for k in range(3)]

            def body(t, _):
                gate, up, dhid = final[GATE, h, t], final[UP, h, t], final[DHID, h, t]
                act, slope = swiglu(gate, up)
                outs[HIDDEN][t] = (act * up).astype(BF16)
                outs[DGATE][t] = (dhid * slope).astype(BF16)
                outs[DUP][t] = (dhid * act).astype(BF16)
                return 0

            lax.fori_loop(0, tiles, body, 0)
        gather_rows((DGATE, DUP, HIDDEN))
        stored = copies_out(gath)
        acc[...] = jnp.zeros_like(acc)

        def body(t, _):
            cols = pl.ds(pl.multiple_of(t * 256, 256), 256)
            g = jnp.concatenate([gath[DGATE, 0, t], gath[DGATE, 1, t]], axis=1)
            u = jnp.concatenate([gath[DUP, 0, t], gath[DUP, 1, t]], axis=1)
            acc[...] += lax.dot_general(g, wg[:, cols], NT_DIMS, preferred_element_type=F32) + lax.dot_general(
                u, wu[:, cols], NT_DIMS, preferred_element_type=F32
            )
            return 0

        lax.fori_loop(0, tiles, body, 0)
        dxp[...] = acc[...].astype(BF16)
        total, sent_z = exchange_cols()
        result = (dy_ref[...].astype(F32) + total).astype(BF16)
        out_ref[...] = result
        blk_out[...] = result
        given = []
        for d in range(n_col):
            c = rcopy(blk_out, dyall.at[my_rows, :], zo_send.at[d], zo_recv.at[d], (0, row, z_peer(d)))
            c.start()
            given.append(c)
        for c in sent + sent_x + sent_z + given:
            c.wait_send()
        for k in range(3):
            rs_drain(k)
            ag_drain(k)
        for c in stored:
            c.wait()

    @pl.when(sec == 0)
    def _():
        sent_x = spread(x_ref, xall, zx_send, zx_recv)
        for c in loads:
            c.wait()
        for c in sent_x:
            c.wait_recv()
        for k in (GATE, UP):
            partials(k)
            rs_start(k, 0)
        reduce_rows((GATE, UP))
        for k in (GATE, UP):
            for h in range(2):
                own = piece(gath, k, h)

                def body(t, _):
                    own[t] = final[k, h, t].astype(BF16)
                    return 0

                lax.fori_loop(0, tiles, body, 0)
        gather_rows((GATE, UP))
        for k in (GATE, UP):
            rs_drain(k)

        for h in range(2):

            def body(t, _):
                gate, up = gath[GATE, h, t].astype(F32), gath[UP, h, t].astype(F32)
                act, slope = swiglu(gate, up)
                part[HIDDEN, h, t] = (act * up).astype(BF16)
                factors[0, h, t] = slope
                factors[1, h, t] = act
                return 0

            lax.fori_loop(0, tiles, body, 0)

        for d in range(n_col):
            rcopy(blk_out, dyall.at[my_rows, :], zo_send.at[d], zo_recv.at[d], (0, row, z_peer(1))).wait_recv()
        partials(DHID)
        rs_start(DHID, 0)
        reduce_rows((DHID,))
        for h in range(2):
            own = piece(gath, DHID, h)

            def body(t, _):
                own[t] = final[DHID, h, t].astype(BF16)
                return 0

            lax.fori_loop(0, tiles, body, 0)
        gather_rows((DHID,))
        rs_drain(DHID)
        acc[...] = jnp.zeros_like(acc)

        def body(t, _):
            cols = pl.ds(pl.multiple_of(t * 256, 256), 256)
            gs, us = [], []
            for h in range(2):
                dh = gath[DHID, h, t].astype(F32)
                gs.append((dh * factors[0, h, t]).astype(BF16))
                us.append((dh * factors[1, h, t]).astype(BF16))
                part[DGATE, h, t] = gs[h]
                part[DUP, h, t] = us[h]
            g = jnp.concatenate(gs, axis=1)
            u = jnp.concatenate(us, axis=1)
            acc[...] += lax.dot_general(g, wg[:, cols], NT_DIMS, preferred_element_type=F32) + lax.dot_general(
                u, wu[:, cols], NT_DIMS, preferred_element_type=F32
            )
            return 0

        lax.fori_loop(0, tiles, body, 0)
        dxp[...] = acc[...].astype(BF16)
        stored = copies_out(part)
        total, sent_z = exchange_cols()
        out_ref[...] = (dyall[my_rows, :].astype(F32) + total).astype(BF16)
        for c in sent_x + sent_z:
            c.wait_send()
        for k in range(3):
            ag_drain(k)
        for c in stored:
            c.wait()


def relay(n_col, x, dy, wg, wu, wd):
    tok_loc, d_loc = x.shape
    f_loc = wg.shape[1]
    tok = tok_loc * n_col
    tiles = f_loc // 256
    blk = tok // RING
    sub = blk // RING
    sem = pltpu.SemaphoreType.DMA
    any_spec = pl.BlockSpec(memory_space=pltpu.HBM)
    vmem_spec = pl.BlockSpec(memory_space=pltpu.VMEM)
    return pl.pallas_call(
        functools.partial(relay_kernel, n_col),
        out_shape=(
            jax.ShapeDtypeStruct((tok_loc, d_loc), BF16),
            jax.ShapeDtypeStruct((3, 2, tiles, tok, 128), BF16),
            jax.ShapeDtypeStruct((tok, d_loc), BF16),
            jax.ShapeDtypeStruct((tok, d_loc), BF16),
        ),
        in_specs=[vmem_spec, vmem_spec, any_spec, any_spec, any_spec],
        out_specs=(vmem_spec, any_spec, any_spec, any_spec),
        scratch_shapes=[
            pltpu.VMEM((d_loc, f_loc), BF16),
            pltpu.VMEM((d_loc, f_loc), BF16),
            pltpu.VMEM((f_loc, d_loc), BF16),
            pltpu.VMEM((tok, d_loc), BF16),
            pltpu.VMEM((tok, d_loc), BF16),
            pltpu.VMEM((3, 2, tiles, tok, 128), BF16),
            pltpu.VMEM((3, 2, 2, tiles, blk // 2, 128), BF16),
            pltpu.VMEM((3, 2, 2, tiles, blk, 128), BF16),
            pltpu.VMEM((3, 2, tiles, sub, 128), BF16),
            pltpu.VMEM((3, 2, 2, tiles, sub, 128), BF16),
            pltpu.VMEM((3, 2, tiles, sub, 128), F32),
            pltpu.VMEM((3, 2, tiles, tok, 128), BF16),
            pltpu.VMEM((2, 2, tiles, tok, 128), F32),
            pltpu.VMEM((tok, d_loc), F32),
            pltpu.VMEM((tok, d_loc), BF16),
            pltpu.VMEM((n_col, tok_loc, d_loc), BF16),
            pltpu.VMEM((tok_loc, d_loc), BF16),
            sem((3,)),
            sem((3,)),
            sem((3, 2, 2, 2, 3)),
            sem((3, 2, 2, 2, 3)),
            sem((3, 2, 2, 2, 3)),
            sem((3, 2, 2, 2, 3)),
            sem((n_col,)),
            sem((n_col,)),
            sem((n_col,)),
            sem((n_col,)),
            sem((n_col,)),
            sem((n_col,)),
            sem((n_col,)),
            sem((n_col,)),
        ],
        compiler_params=pltpu.CompilerParams(
            collective_id=0, has_side_effects=True, vmem_limit_bytes=48 * 1024 * 1024
        ),
        name="relay",
    )(x, dy, wg, wu, wd)


def weight_kernel(h_ref, x_ref, dy_ref, gate_ref, up_ref, down_ref):
    hid = jnp.concatenate([h_ref[HIDDEN, 0, 0], h_ref[HIDDEN, 1, 0]], axis=1)
    g = jnp.concatenate([h_ref[DGATE, 0, 0], h_ref[DGATE, 1, 0]], axis=1)
    u = jnp.concatenate([h_ref[DUP, 0, 0], h_ref[DUP, 1, 0]], axis=1)
    gate_ref[...] = lax.dot_general(x_ref[...], g, TN_DIMS, preferred_element_type=F32)
    up_ref[...] = lax.dot_general(x_ref[...], u, TN_DIMS, preferred_element_type=F32)
    down_ref[...] = lax.dot_general(hid, dy_ref[...], TN_DIMS, preferred_element_type=F32)


def weight_grads(h, x, dy):
    tiles, tok = h.shape[2:4]
    d_loc = x.shape[1]
    whole = pl.BlockSpec((tok, d_loc), lambda t: (0, 0))
    wide = pl.BlockSpec((d_loc, 256), lambda t: (0, t))
    return pl.pallas_call(
        weight_kernel,
        grid=(tiles,),
        out_shape=(
            jax.ShapeDtypeStruct((d_loc, tiles * 256), F32),
            jax.ShapeDtypeStruct((d_loc, tiles * 256), F32),
            jax.ShapeDtypeStruct((tiles * 256, d_loc), F32),
        ),
        in_specs=[pl.BlockSpec((3, 2, 1, tok, 128), lambda t: (0, 0, t, 0, 0)), whole, whole],
        out_specs=(wide, wide, pl.BlockSpec((256, d_loc), lambda t: (t, 0))),
        name="weight_grads",
    )(h, x, dy)


def shards(section_inputs, out_grad, gate_weight, up_weight, down_weight):
    n_col = lax.axis_size("col")
    panels = section_inputs[0]
    merged = (panels.shape[0] * panels.shape[1], panels.shape[2])
    x = panels.reshape(merged)
    dy = out_grad.reshape(merged)
    out, h, x_all, dy_all = relay(n_col, x, dy, gate_weight[0], up_weight[0], down_weight[0])
    gate, up, down = weight_grads(h, x_all, dy_all)
    return out.reshape(panels.shape)[None], gate[None], up[None], down[None]


def solution(mesh):
    return jax.shard_map(
        shards,
        mesh=mesh,
        in_specs=(
            P("section", None, "col", "row"),
            P(None, "col", "row"),
            P("section", "row", "col"),
            P("section", "row", "col"),
            P("section", "col", "row"),
        ),
        out_specs=(
            P("section", None, "col", "row"),
            P("section", "row", "col"),
            P("section", "row", "col"),
            P("section", "col", "row"),
        ),
        check_vma=False,
    )
```
